256 devices in a mesh: ta: 4 (over z_hi), sa: 64 (over y, z_lo, x, core).
Axes of the slice: x: 4, y: 4, z: 8 (z_hi: 4, z_lo: 2; z = z_hi * 2 + z_lo), core: 2. Of those that a mesh axis runs over, the one named last changes fastest.
Arguments:
- frames: float32 [16, 64, 64, 4096], P('ta', 'sa'), may hold values from -6 to 6
- taps: float32 [7], replicated, may hold values from 0.1 to 0.3
Outputs:
- columns: float32 [64, 16, 512, 512], P('sa', 'ta')
The draws below stay inside these ranges and needn't reach their ends.
All inputs are finite; a program needn't handle non-finite values.
Results may differ from the reference program's by a relative error of at most 0.00002.
Values sent between devices are 32-bit elements; how exact they have to be, the bound alone decides.
A program may use at most 128 MiB of HBM per device.

```python
import jax
import jax.numpy as jnp
from jax import lax

NY = 4096
NX = 4096
TS = 512
TIME = 16
READERS = 64
STRIP = 64
TILES = 64
N_SA = 64


def level_of(rng, extent, cuts, low, high):
    gain = 1.0
    for axis_at, blocks in cuts:
        heights = jax.random.uniform(jax.random.fold_in(jax.random.fold_in(rng, 6), axis_at), (blocks,), jnp.float32, low / len(cuts), high / len(cuts))
        gain = gain * jnp.repeat(jnp.exp(heights), extent[axis_at] // blocks).reshape((-1,) + (1,) * (len(extent) - 1 - axis_at))
    return gain


def normal_values(stream_key, shape, deviation, limit, pieces=(), kind=jnp.bfloat16):
    result = deviation * jax.random.normal(stream_key, shape, jnp.float32)
    if pieces:
        result = result * level_of(stream_key, shape, pieces, -0.22, 0.18)
    return jnp.clip(result, -limit, limit).astype(kind)


def setup_inputs(seed: int = 0) -> dict:
    seeds = jax.random.split(jax.random.key(seed), 3)
    return {
        "frames": normal_values(seeds[0], (TIME, READERS, STRIP, NX), 1.0, 6.0, ((0, 4), (1, 64)), jnp.float32),
        "taps": jnp.clip(jax.random.uniform(seeds[1], (7,), jnp.float32, 0.1, 0.3), 0.1, 0.3),
    }


def reference(frames, taps):
    per_tile = TS // N_SA
    tile_rows = NY // TS
    tile_cols = NX // TS

    def one_row(index):
        piece = lax.dynamic_slice_in_dim(frames, index * per_tile, per_tile, 2)
        field = piece.transpose(0, 2, 1, 3).reshape(TIME, TS, NX)
        padded = jnp.pad(field, ((3, 3), (0, 0), (0, 0)))
        total = jnp.zeros_like(field)
        for offset in range(7):
            total = total + taps[offset] * padded[offset:offset + TIME]
        return total.reshape(TIME, TS, tile_cols, TS).transpose(2, 0, 1, 3)

    stacked = lax.map(one_row, jnp.arange(tile_rows, dtype=jnp.int32))
    return stacked.reshape(TILES, TIME, TS, TS)
```

```python
import functools

import jax
import jax.numpy as jnp
from jax import lax
from jax.experimental import pallas as pl
from jax.experimental.pallas import tpu as pltpu
from jax.sharding import PartitionSpec as P

TS = 512
NX = 4
NYC = 4
SLOTS = NX * NYC * 2
OFFSETS = (
    (0, 0), (1, 0), (0, 1), (3, 0), (0, 3), (1, 1), (3, 3), (1, 3),
    (3, 1), (2, 0), (0, 2), (2, 1), (1, 2), (2, 3), (3, 2), (2, 2),
)
LAG_HALO = 3
LAG_FWD = 8


def kernel(
    groups, taps_ref, frames, out, plane, cross, halo, total,
    own_sem, in_send, in_recv, x_send, x_recv, h_send, h_recv, out_sem,
):
    g = lax.axis_index("ta")
    s = lax.axis_index("sa")
    c = s % 2
    x = (s // 2) % NX
    a = (s // (2 * NX)) % 2
    y = s // (4 * NX)
    mine = (y * NX + x) * 2 + c
    last = groups - 1

    def device(group, yy, zz, xx, cc):
        return (group, ((yy * 2 + zz) * NX + xx) * 2 + cc)

    def chip(k, sign):
        dx, dy = OFFSETS[k]
        return (x + (dx if sign > 0 else NX - dx)) % NX, (y + (dy if sign > 0 else NYC - dy)) % NYC

    step = 2 * a - 1
    beyond = g + step
    has_up = g < last
    has_down = g > 0
    has_beyond = jnp.logical_and(beyond >= 0, beyond <= last)

    def piece(xx, yy, cc):
        return frames.at[:, pl.ds(2 * yy, 2), :, pl.ds(pl.multiple_of(TS * (2 * xx + cc), TS), TS)]

    own = pltpu.make_async_copy(piece(x, y, c), plane.at[mine], own_sem)
    own.start()

    barrier = pltpu.get_barrier_semaphore()

    def greet(target):
        pl.semaphore_signal(barrier, inc=1, device_id=target, device_id_type=pl.DeviceIdType.MESH)

    for k in range(len(OFFSETS)):
        xx, yy = chip(k, 1)
        for other in range(2):
            cc = (c + 1 - other) % 2
            if k == 0 and other == 1:
                continue
            greet(device(g, yy, a, xx, cc))
    greet(device(g, y, 1 - a, x, c))

    @pl.when(has_up)
    def _():
        greet(device(g + 1, y, a, x, c))

    @pl.when(has_down)
    def _():
        greet(device(g - 1, y, a, x, c))

    @pl.when(has_beyond)
    def _():
        greet(device(beyond, y, 1 - a, x, c))

    count = (
        2 * len(OFFSETS) - 1 + 1 + has_up.astype(jnp.int32)
        + has_down.astype(jnp.int32) + has_beyond.astype(jnp.int32)
    )
    pl.semaphore_wait(barrier, count)

    def in_plane(k, other):
        xx, yy = chip(k, 1)
        cc = (c + 1 - other) % 2
        return pltpu.make_async_remote_copy(
            src_ref=piece(xx, yy, cc), dst_ref=plane.at[mine],
            send_sem=in_send.at[2 * k + other], recv_sem=in_recv.at[mine],
            device_id=device(g, yy, a, xx, cc), device_id_type=pl.DeviceIdType.MESH,
        )

    def arrival(slot):
        return pltpu.make_async_remote_copy(
            src_ref=piece(x, y, c), dst_ref=plane.at[slot],
            send_sem=in_send.at[0], recv_sem=in_recv.at[slot],
            device_id=device(g, y, 1 - a, x, c), device_id_type=pl.DeviceIdType.MESH,
        )

    for k in range(len(OFFSETS)):
        for other in range(2):
            if k == 0 and other == 1:
                continue
            in_plane(k, other).start()

    def zero(side):
        def body(i, _):
            halo[side, i // SLOTS, i % SLOTS] = jnp.zeros((3, 8, TS), jnp.float32)
            return 0
        lax.fori_loop(0, 2 * SLOTS, body, 0)

    @pl.when(jnp.logical_not(has_down))
    def _():
        zero(0)

    @pl.when(jnp.logical_not(has_up))
    def _():
        zero(1)

    def chip_of(k):
        xx, yy = chip(k, -1)
        return yy * NX + xx

    def cross_copy(k):
        m = chip_of(k)
        return pltpu.make_async_remote_copy(
            src_ref=plane.at[pl.ds(2 * m, 2), :, 1 - a], dst_ref=cross.at[pl.ds(2 * m, 2)],
            send_sem=x_send.at[m], recv_sem=x_recv.at[m],
            device_id=device(g, y, 1 - a, x, c), device_id_type=pl.DeviceIdType.MESH,
        )

    def halo_copy(k, src, start, side, rel, target):
        m = chip_of(k)
        return pltpu.make_async_remote_copy(
            src_ref=src, dst_ref=halo.at[side, rel, pl.ds(2 * m, 2)],
            send_sem=h_send.at[side, rel, m], recv_sem=h_recv.at[side, rel, m],
            device_id=target, device_id_type=pl.DeviceIdType.MESH,
        )

    def up(k):
        m = chip_of(k)
        return halo_copy(k, plane.at[pl.ds(2 * m, 2), pl.ds(1, 3), a], 1, 0, 0, device(g + 1, y, a, x, c))

    def down(k):
        m = chip_of(k)
        return halo_copy(k, plane.at[pl.ds(2 * m, 2), pl.ds(0, 3), a], 0, 1, 0, device(g - 1, y, a, x, c))

    def side_copy(k):
        m = chip_of(k)
        return pltpu.make_async_remote_copy(
            src_ref=plane.at[pl.ds(2 * m, 2), pl.ds(a, 3), 1 - a],
            dst_ref=halo.at[1 - a, 1, pl.ds(2 * m, 2)],
            send_sem=h_send.at[a, 1, m], recv_sem=h_recv.at[1 - a, 1, m],
            device_id=device(beyond, y, 1 - a, x, c), device_id_type=pl.DeviceIdType.MESH,
        )

    def forward(k):
        m = chip_of(k)
        return pltpu.make_async_remote_copy(
            src_ref=cross.at[pl.ds(2 * m, 2), pl.ds(a, 3)],
            dst_ref=halo.at[1 - a, 1, pl.ds(2 * m, 2)],
            send_sem=h_send.at[1 - a, 1, m], recv_sem=h_recv.at[1 - a, 1, m],
            device_id=device(beyond, y, a, x, c), device_id_type=pl.DeviceIdType.MESH,
        )

    def start_if(flag, make):
        @pl.when(flag)
        def _():
            make().start()

    n = len(OFFSETS)
    for k in range(n + max(LAG_HALO, LAG_FWD)):
        if k < n:
            m = chip_of(k)
            if k == 0:
                own.wait()
                arrival(2 * m + 1 - c).wait_recv()
            else:
                arrival(2 * m).wait_recv()
                arrival(2 * m + 1).wait_recv()
            cross_copy(k).start()
            start_if(has_beyond, lambda: side_copy(k))
        if 0 <= k - LAG_HALO < n:
            start_if(has_up, lambda: up(k - LAG_HALO))
            start_if(has_down, lambda: down(k - LAG_HALO))
        if 0 <= k - LAG_FWD < n:
            cross_copy(k - LAG_FWD).wait_recv()
            start_if(has_beyond, lambda: forward(k - LAG_FWD))

    taps = [taps_ref[j] for j in range(7)]

    def out_copy(k, rel):
        m = chip_of(k)
        z = a if rel == 0 else 1 - a
        row = (m // NX) * 4 * NX + z * 2 * NX + (m % NX) * 2
        return pltpu.make_async_copy(
            total.at[:, pl.ds(row, 2)], out.at[:, pl.ds(row, 2)], out_sem.at[rel, m]
        )

    def sum_rows(k, rel):
        m = chip_of(k)
        z = a if rel == 0 else 1 - a
        row = (m // NX) * 4 * NX + z * 2 * NX + (m % NX) * 2
        for i in range(2):
            slot = 2 * m + i
            values = [halo[0, rel, slot, j] for j in range(3)]
            if rel == 0:
                values += [plane[slot, j, a] for j in range(4)]
            else:
                values += [cross[slot, j] for j in range(4)]
            values += [halo[1, rel, slot, j] for j in range(3)]
            for t in range(4):
                acc = taps[0] * values[t]
                for j in range(1, 7):
                    acc = acc + taps[j] * values[t + j]
                total[t, row + i] = acc

    for rel in range(2):
        for k in range(n):
            m = chip_of(k)
            for side, flag in ((0, has_down), (1, has_up)):
                @pl.when(flag)
                def _():
                    halo_copy(
                        k, plane.at[pl.ds(2 * m, 2), pl.ds(0, 3), a], 0, side, rel,
                        device(g, y, 1 - a, x, c),
                    ).wait_recv()
            sum_rows(k, rel)
            out_copy(k, rel).start()

    for k in range(n):
        for other in range(2):
            if k == 0 and other == 1:
                continue
            in_plane(k, other).wait_send()
        cross_copy(k).wait_send()

        @pl.when(has_up)
        def _():
            up(k).wait_send()

        @pl.when(has_down)
        def _():
            down(k).wait_send()

        @pl.when(has_beyond)
        def _():
            side_copy(k).wait_send()
            forward(k).wait_send()
        out_copy(k, 0).wait()
        out_copy(k, 1).wait()


def on_device(groups, frames, taps):
    shaped = frames.reshape(4, 8, 8, frames.shape[3])
    chips = NX * NYC
    summed = pl.pallas_call(
        functools.partial(kernel, groups),
        out_shape=jax.ShapeDtypeStruct((4, 2 * SLOTS, 8, TS), jnp.float32),
        in_specs=[pl.BlockSpec(memory_space=pltpu.SMEM), pl.BlockSpec(memory_space=pl.ANY)],
        out_specs=pl.BlockSpec(memory_space=pl.ANY),
        scratch_shapes=[
            pltpu.VMEM((SLOTS, 4, 2, 8, TS), jnp.float32),
            pltpu.VMEM((SLOTS, 4, 8, TS), jnp.float32),
            pltpu.VMEM((2, 2, SLOTS, 3, 8, TS), jnp.float32),
            pltpu.VMEM((4, 2 * SLOTS, 8, TS), jnp.float32),
            pltpu.SemaphoreType.DMA,
            pltpu.SemaphoreType.DMA((SLOTS,)),
            pltpu.SemaphoreType.DMA((SLOTS,)),
            pltpu.SemaphoreType.DMA((chips,)),
            pltpu.SemaphoreType.DMA((chips,)),
            pltpu.SemaphoreType.DMA((2, 2, chips)),
            pltpu.SemaphoreType.DMA((2, 2, chips)),
            pltpu.SemaphoreType.DMA((2, chips)),
        ],
        compiler_params=pltpu.CompilerParams(collective_id=0, has_side_effects=True),
        name="exchange",
    )(taps, shaped)
    return summed.transpose(0, 2, 1, 3).reshape(1, 4, TS, TS)


def solution(mesh):
    placed = (P("ta", "sa", None, None), P())
    return jax.shard_map(
        functools.partial(on_device, mesh.shape["ta"]),
        mesh=mesh, in_specs=placed, out_specs=P("sa", "ta", None, None), check_vma=False,
    )
```

```python
import functools

import jax
import jax.numpy as jnp
from jax import lax
from jax.experimental import pallas as pl
from jax.experimental.pallas import tpu as pltpu
from jax.sharding import PartitionSpec as P

TS = 512
NX = 4
CHIPS = NX * NX
SLOTS = 2 * CHIPS
MESH = pl.DeviceIdType.MESH

UNITS = (
    ('one', 0, 0),
    ('one', 0, 1),
    ('one', 1, 0),
    ('one', 4, 0),
    ('one', 3, 0),
    ('one', 12, 0),
    ('one', 1, 1),
    ('one', 4, 1),
    ('one', 3, 1),
    ('one', 12, 1),
    ('chip', 5),
    ('chip', 13),
    ('chip', 2),
    ('pair', 8),
    ('pair', 6),
    ('pair', 14),
    ('pair', 10),
)
SENDS = (
    (0, 1),
    (1, 0),
    (4, 0),
    (3, 0),
    (12, 0),
    (1, 1),
    (4, 1),
    (3, 1),
    (12, 1),
    (5, 0),
    (5, 1),
    (13, 0),
    (13, 1),
    (2, 0),
    (2, 1),
    (8, 0),
    (8, 1),
    (9, 0),
    (9, 1),
    (6, 0),
    (6, 1),
    (7, 0),
    (7, 1),
    (14, 0),
    (14, 1),
    (15, 0),
    (15, 1),
    (10, 0),
    (10, 1),
    (11, 0),
    (11, 1),
)
SIZES = {"one": 1, "chip": 2, "pair": 4}
STEPS = len(UNITS)
LAGS = dict(P=0, S1=0, Nf=0, N=0, F=3, R1=4, R3=2, X=37, W=37, A=31, R2=39, B=65)
ORDER = tuple(
    (kind, step - lag)
    for step in range(STEPS + max(LAGS.values()))
    for kind, lag in LAGS.items()
    if 0 <= step - lag < STEPS
)


def unit_of(offset, other):
    for u, unit in enumerate(UNITS):
        if unit[0] == "one":
            hit = unit[1:] == (offset, other)
        elif unit[0] == "chip":
            hit = unit[1] == offset
        else:
            hit = unit[1] // 2 == offset // 2
        if hit:
            return u


def flipped(v, bits):
    return (v, v + 1 - 2 * (v % 2), (v + 2) % NX, NX - 1 - v)[bits]


def kernel(
    groups, taps_hbm, frames, out, taps_ref, plane, cross, relay, halo,
    taps_sem, own_sem, in_send, in_recv, x_recv, z_send, r_recv, h_recv,
):
    g = lax.axis_index("ta")
    s = lax.axis_index("sa")
    c = s % 2
    x = (s // 2) % NX
    a = (s // (2 * NX)) % 2
    y = s // (4 * NX)
    mine = (y * NX + x) * 2 + c
    last = groups - 1
    step = 2 * a - 1
    beyond, near = g + step, g - step
    has_near = jnp.logical_and(near >= 0, near <= last)
    has_far = jnp.logical_and(beyond >= 0, beyond <= last)
    has_up = g < last
    has_down = g > 0

    def device(group, yy, zz, xx, cc):
        return (group, ((yy * 2 + zz) * NX + xx) * 2 + cc)

    def chip(offset):
        return flipped(y, offset // NX), flipped(x, offset % NX)

    partner = device(g, y, 1 - a, x, c)
    beyond_chip = device(beyond, y, 1 - a, x, c)

    def slots(u):
        unit = UNITS[u]
        yy, xx = chip(unit[1])
        base = 2 * (yy * NX + xx)
        if unit[0] == "one":
            return pl.ds(base + (c if unit[2] == 0 else 1 - c), 1)
        if unit[0] == "pair":
            base = base // 4 * 4
        return pl.ds(base, SIZES[unit[0]])

    def piece(yy, xx, cc):
        return frames.at[:, pl.ds(2 * yy, 2), :, pl.ds(pl.multiple_of(TS * (2 * xx + cc), TS), TS)]

    own = pltpu.make_async_copy(piece(y, x, c), plane.at[mine], own_sem)
    own.start()
    weights = pltpu.make_async_copy(taps_hbm, taps_ref, taps_sem)
    weights.start()

    barrier = pltpu.get_barrier_semaphore()

    def greet(target):
        pl.semaphore_signal(barrier, inc=1, device_id=target, device_id_type=MESH)

    for offset, other in reversed(SENDS):
        yy, xx = chip(offset)
        greet(device(g, yy, a, xx, (c + other) % 2))
    greet(partner)

    @pl.when(has_far)
    def _():
        greet(beyond_chip)

    pl.semaphore_wait(barrier, SLOTS + has_far.astype(jnp.int32))

    def remote(src, dst, send, recv, target):
        return pltpu.make_async_remote_copy(
            src_ref=src, dst_ref=dst, send_sem=send, recv_sem=recv,
            device_id=target, device_id_type=MESH,
        )

    def in_plane(offset, other):
        yy, xx = chip(offset)
        cc = (c + other) % 2
        return remote(
            piece(yy, xx, cc), plane.at[mine], in_send, in_recv.at[unit_of(offset, other)],
            device(g, yy, a, xx, cc),
        )

    def cross_copy(u):
        return remote(
            plane.at[slots(u), :, 1 - a], cross.at[slots(u)], z_send.at[7], x_recv.at[u], partner
        )

    def near_halo(u):
        return remote(
            plane.at[slots(u), pl.ds(1 - a, 3), a], relay.at[0, slots(u)],
            z_send.at[0], r_recv.at[0, u], partner,
        )

    def far_halo(u):
        return remote(
            plane.at[slots(u), pl.ds(a, 3), a], relay.at[1, slots(u)],
            z_send.at[1], r_recv.at[1, u], beyond_chip,
        )

    def side_halo(u):
        return remote(
            plane.at[slots(u), pl.ds(a, 3), 1 - a], halo.at[1 - a, 1, slots(u)],
            z_send.at[2], h_recv.at[1 - a, 1, u], beyond_chip,
        )

    def forward(u):
        return remote(
            cross.at[slots(u), pl.ds(a, 3)], relay.at[2, slots(u)],
            z_send.at[3], r_recv.at[2, u], beyond_chip,
        )

    def relay_near(u, w):
        return remote(
            relay.at[1 + w, slots(u)], halo.at[a, w, slots(u)],
            z_send.at[4 + w], h_recv.at[a, w, u], partner,
        )

    def relay_far(u):
        return remote(
            relay.at[0, slots(u)], halo.at[1 - a, 0, slots(u)],
            z_send.at[6], h_recv.at[1 - a, 0, u], beyond_chip,
        )

    def wait_in(ref, sem):
        remote(ref, ref, in_send, sem, partner).wait_recv()

    def wait_out(ref, sem):
        remote(ref, ref, sem, own_sem, partner).wait_send()


    for offset, other in SENDS:
        in_plane(offset, other).start()

    def zero(side):
        def body(i, _):
            halo[side, i // SLOTS, i % SLOTS] = jnp.zeros((3, 8, TS), jnp.float32)
            return 0
        lax.fori_loop(0, 2 * SLOTS, body, 0)

    @pl.when(jnp.logical_not(has_down))
    def _():
        zero(0)

    @pl.when(jnp.logical_not(has_up))
    def _():
        zero(1)

    weights.wait()
    taps = [taps_ref[j] for j in range(7)]

    def sum_rows(u, rel):
        run = slots(u)

        def body(i, _):
            slot = run.start + i
            m = slot // 2
            z = a if rel == 0 else 1 - a
            row = ((m // NX) * 2 + z) * 32 + (m % NX) * 2 + slot % 2
            for q in range(TS // 128):
                lanes = pl.ds(q * 128, 128)
                values = [halo[0, rel, slot, j, :, lanes] for j in range(3)]
                if rel == 0:
                    values += [plane[slot, j, a, :, lanes] for j in range(4)]
                else:
                    values += [cross[slot, j, :, lanes] for j in range(4)]
                values += [halo[1, rel, slot, j, :, lanes] for j in range(3)]
                for t in range(4):
                    acc = taps[0] * values[t]
                    for j in range(1, 7):
                        acc = acc + taps[j] * values[t + j]
                    out[t, pl.ds(row + 8 * q, 8, stride=TS // 8 * 4), :] = acc
            return 0

        lax.fori_loop(0, run.size, body, 0)

    def finish(u, rel):
        for side, flag in ((0, has_down), (1, has_up)):
            @pl.when(flag)
            def _():
                wait_in(halo.at[side, rel, slots(u)], h_recv.at[side, rel, u])
        sum_rows(u, rel)

    for kind, u in ORDER:
        if kind == "P":
            if u == 0:
                own.wait()
            else:
                wait_in(plane.at[slots(u)], in_recv.at[u])
        elif kind == "S1":
            cross_copy(u).start()
        elif kind == "N":
            @pl.when(has_near)
            def _():
                near_halo(u).start()
        elif kind == "A":
            finish(u, 0)
        elif kind == "X":
            wait_in(cross.at[slots(u)], x_recv.at[u])
        elif kind == "B":
            finish(u, 1)
        else:
            @pl.when(has_far)
            def _():
                if kind == "Nf":
                    far_halo(u).start()
                elif kind == "F":
                    side_halo(u).start()
                elif kind == "W":
                    forward(u).start()
                elif kind == "R1":
                    wait_in(relay.at[1, slots(u)], r_recv.at[1, u])
                    relay_near(u, 0).start()
                elif kind == "R2":
                    wait_in(relay.at[2, slots(u)], r_recv.at[2, u])
                    relay_near(u, 1).start()
                elif kind == "R3":
                    wait_in(relay.at[0, slots(u)], r_recv.at[0, u])
                    relay_far(u).start()

    wait_out(plane.at[pl.ds(0, SLOTS - 1)], in_send)
    wait_out(cross, z_send.at[7])

    @pl.when(has_near)
    def _():
        wait_out(relay.at[0], z_send.at[0])

    @pl.when(has_far)
    def _():
        for kind in range(1, 7):
            wait_out(relay.at[0], z_send.at[kind])


def on_device(groups, frames, taps):
    shaped = frames.reshape(4, 8, 8, frames.shape[3])
    summed = pl.pallas_call(
        functools.partial(kernel, groups),
        out_shape=jax.ShapeDtypeStruct((4, 4 * TS, 128), jnp.float32),
        in_specs=[pl.BlockSpec(memory_space=pltpu.HBM), pl.BlockSpec(memory_space=pltpu.HBM)],
        out_specs=pl.BlockSpec(memory_space=pltpu.VMEM),
        scratch_shapes=[
            pltpu.SMEM((7,), jnp.float32),
            pltpu.VMEM((SLOTS, 4, 2, 8, TS), jnp.float32),
            pltpu.VMEM((SLOTS, 4, 8, TS), jnp.float32),
            pltpu.VMEM((3, SLOTS, 3, 8, TS), jnp.float32),
            pltpu.VMEM((2, 2, SLOTS, 3, 8, TS), jnp.float32),
            pltpu.SemaphoreType.DMA,
            pltpu.SemaphoreType.DMA,
            pltpu.SemaphoreType.DMA,
            pltpu.SemaphoreType.DMA((STEPS,)),
            pltpu.SemaphoreType.DMA((STEPS,)),
            pltpu.SemaphoreType.DMA((8,)),
            pltpu.SemaphoreType.DMA((3, STEPS)),
            pltpu.SemaphoreType.DMA((2, 2, STEPS)),
        ],
        compiler_params=pltpu.CompilerParams(
            collective_id=0, has_side_effects=True, vmem_limit_bytes=24 * 2**20
        ),
        name="exchange",
    )(
        pltpu.with_memory_space_constraint(taps, pltpu.HBM),
        pltpu.with_memory_space_constraint(shaped, pltpu.HBM),
    )
    tiled = summed.reshape(4, TS // 8, TS // 128, 8, 128)
    return tiled.transpose(0, 1, 3, 2, 4).reshape(1, 4, TS, TS)


def solution(mesh):
    placed = (P("ta", "sa", None, None), P())
    return jax.shard_map(
        functools.partial(on_device, mesh.shape["ta"]),
        mesh=mesh, in_specs=placed, out_specs=P("sa", "ta", None, None), check_vma=False,
    )
```

```python
import functools

import jax
import jax.numpy as jnp
from jax import lax
from jax.experimental import pallas as pl
from jax.experimental.pallas import tpu as pltpu
from jax.sharding import PartitionSpec as P

TS = 512
NX = 4
CHIPS = NX * NX
SLOTS = 2 * CHIPS
MESH = pl.DeviceIdType.MESH

UNITS = (
    ('one', 0, 0),
    ('one', 0, 1),
    ('one', 1, 0),
    ('one', 4, 0),
    ('one', 3, 0),
    ('one', 12, 0),
    ('one', 1, 1),
    ('one', 4, 1),
    ('one', 3, 1),
    ('one', 12, 1),
    ('chip', 5),
    ('chip', 13),
    ('chip', 2),
    ('pair', 8),
    ('pair', 6),
    ('pair', 14),
    ('pair', 10),
)
SENDS = (
    (0, 1),
    (1, 0),
    (4, 0),
    (3, 0),
    (12, 0),
    (1, 1),
    (4, 1),
    (3, 1),
    (12, 1),
    (5, 0),
    (5, 1),
    (13, 0),
    (13, 1),
    (2, 0),
    (2, 1),
    (8, 0),
    (8, 1),
    (9, 0),
    (9, 1),
    (6, 0),
    (6, 1),
    (7, 0),
    (7, 1),
    (14, 0),
    (14, 1),
    (15, 0),
    (15, 1),
    (10, 0),
    (10, 1),
    (11, 0),
    (11, 1),
)
CLOSE = tuple(t for t in SENDS if t[0] // 4 == 0 or t[0] % 4 == 0)
SIZES = {"one": 1, "chip": 2, "pair": 4}
STEPS = len(UNITS)
GROUPS = (tuple(range(2, 10)), (0, 1, 10, 11), (12, 13), (14,), (15,), (16,))
GROUP_OF = {u: i for i, units in enumerate(GROUPS) for u in units}
LAGS = dict(P=0, S1=0, Nf=0, N=0, F=0, R1=1, R3=35, X=4, W=4, R2=14, A=50, B=58)
ORDER = tuple(
    (kind, step - lag)
    for step in range(STEPS + max(LAGS.values()))
    for kind, lag in LAGS.items()
    if 0 <= step - lag < (len(GROUPS) if kind in "AB" else STEPS)
    and (step > lag or kind not in ("P", "S1", "N", "Nf", "F"))
)


def unit_of(offset, other):
    for u, unit in enumerate(UNITS):
        if unit[0] == "one":
            hit = unit[1:] == (offset, other)
        elif unit[0] == "chip":
            hit = unit[1] == offset
        else:
            hit = unit[1] // 2 == offset // 2
        if hit:
            return u


def flipped(v, bits):
    return (v, v + 1 - 2 * (v % 2), (v + 2) % NX, NX - 1 - v)[bits]


def kernel(
    groups, taps_hbm, frames, out, taps_ref, plane, cross, relay, halo,
    taps_sem, own_sem, row_sem, in_send, in_recv, x_recv, z_send, r_recv, h_recv,
):
    g = lax.axis_index("ta")
    s = lax.axis_index("sa")
    c = s % 2
    x = (s // 2) % NX
    a = (s // (2 * NX)) % 2
    y = s // (4 * NX)
    mine = (y * NX + x) * 2 + c
    last = groups - 1
    step = 2 * a - 1
    beyond, near = g + step, g - step
    has_near = jnp.logical_and(near >= 0, near <= last)
    has_far = jnp.logical_and(beyond >= 0, beyond <= last)
    has_up = g < last
    has_down = g > 0

    def device(group, yy, zz, xx, cc):
        return (group, ((yy * 2 + zz) * NX + xx) * 2 + cc)

    def chip(offset):
        return flipped(y, offset // NX), flipped(x, offset % NX)

    partner = device(g, y, 1 - a, x, c)
    beyond_chip = device(beyond, y, 1 - a, x, c)

    def slots(u):
        unit = UNITS[u]
        yy, xx = chip(unit[1])
        base = 2 * (yy * NX + xx)
        if unit[0] == "one":
            return pl.ds(base + (c if unit[2] == 0 else 1 - c), 1)
        if unit[0] == "pair":
            base = base // 4 * 4
        return pl.ds(base, SIZES[unit[0]])

    def piece(yy, xx, cc):
        return frames.at[:, pl.ds(2 * yy, 2), :, pl.ds(pl.multiple_of(TS * (2 * xx + cc), TS), TS)]

    own = pltpu.make_async_copy(piece(y, x, c), plane.at[mine], own_sem)
    own.start()
    weights = pltpu.make_async_copy(taps_hbm, taps_ref, taps_sem)
    weights.start()

    barrier = pltpu.get_barrier_semaphore()

    def signal(semaphore, target):
        pl.semaphore_signal(semaphore, inc=1, device_id=target, device_id_type=MESH)

    for offset, other in reversed(CLOSE):
        yy, xx = chip(offset)
        signal(barrier, device(g, yy, a, xx, (c + other) % 2))
    signal(barrier, partner)

    @pl.when(has_far)
    def _():
        signal(barrier, beyond_chip)

    pl.semaphore_wait(barrier, len(CLOSE) + 1 + has_far.astype(jnp.int32))

    def remote(src, dst, send, recv, target):
        return pltpu.make_async_remote_copy(
            src_ref=src, dst_ref=dst, send_sem=send, recv_sem=recv,
            device_id=target, device_id_type=MESH,
        )

    def in_plane(offset, other):
        yy, xx = chip(offset)
        cc = (c + other) % 2
        return remote(
            piece(yy, xx, cc), plane.at[mine], in_send, in_recv.at[unit_of(offset, other)],
            device(g, yy, a, xx, cc),
        )

    def cross_copy(u):
        return remote(
            plane.at[slots(u), :, 1 - a], cross.at[slots(u)], z_send.at[7], x_recv.at[u], partner
        )

    def near_halo(u):
        return remote(
            plane.at[slots(u), pl.ds(1 - a, 3), a], relay.at[0, slots(u)],
            z_send.at[0], r_recv.at[0, u], partner,
        )

    def far_halo(u):
        return remote(
            plane.at[slots(u), pl.ds(a, 3), a], relay.at[1, slots(u)],
            z_send.at[1], r_recv.at[1, u], beyond_chip,
        )

    def side_halo(u):
        return remote(
            plane.at[slots(u), pl.ds(a, 3), 1 - a], halo.at[1 - a, 1, slots(u)],
            z_send.at[2], h_recv.at[1 - a, 1, GROUP_OF[u]], beyond_chip,
        )

    def forward(u):
        return remote(
            cross.at[slots(u), pl.ds(a, 3)], relay.at[2, slots(u)],
            z_send.at[3], r_recv.at[2, u], beyond_chip,
        )

    def relay_near(u, w):
        return remote(
            relay.at[1 + w, slots(u)], halo.at[a, w, slots(u)],
            z_send.at[4 + w], h_recv.at[a, w, GROUP_OF[u]], partner,
        )

    def relay_far(u):
        return remote(
            relay.at[0, slots(u)], halo.at[1 - a, 0, slots(u)],
            z_send.at[6], h_recv.at[1 - a, 0, GROUP_OF[u]], beyond_chip,
        )

    def wait_in(ref, sem):
        remote(ref, ref, in_send, sem, partner).wait_recv()

    def wait_out(ref, sem):
        remote(ref, ref, sem, own_sem, partner).wait_send()


    for offset, other in CLOSE:
        in_plane(offset, other).start()
    for bits in range(1, NX):
        signal(row_sem, device(g, y, a, flipped(x, bits), c))

    own.wait()
    cross_copy(0).start()

    @pl.when(has_near)
    def _():
        near_halo(0).start()

    @pl.when(has_far)
    def _():
        far_halo(0).start()
        side_halo(0).start()

    pl.semaphore_wait(row_sem, NX - 1)
    for offset, other in SENDS:
        if (offset, other) not in CLOSE:
            in_plane(offset, other).start()

    def zero(side):
        def body(i, _):
            halo[side, i // SLOTS, i % SLOTS] = jnp.zeros((3, 8, TS), jnp.float32)
            return 0
        lax.fori_loop(0, 2 * SLOTS, body, 0)

    @pl.when(jnp.logical_not(has_down))
    def _():
        zero(0)

    @pl.when(jnp.logical_not(has_up))
    def _():
        zero(1)

    weights.wait()
    taps = [taps_ref[j] for j in range(7)]

    def sum_rows(u, rel):
        run = slots(u)

        def body(i, _):
            slot = run.start + i
            m = slot // 2
            z = a if rel == 0 else 1 - a
            row = ((m // NX) * 2 + z) * 32 + (m % NX) * 2 + slot % 2
            for q in range(TS // 128):
                lanes = pl.ds(q * 128, 128)
                values = [halo[0, rel, slot, j, :, lanes] for j in range(3)]
                if rel == 0:
                    values += [plane[slot, j, a, :, lanes] for j in range(4)]
                else:
                    values += [cross[slot, j, :, lanes] for j in range(4)]
                values += [halo[1, rel, slot, j, :, lanes] for j in range(3)]
                for t in range(4):
                    acc = taps[0] * values[t]
                    for j in range(1, 7):
                        acc = acc + taps[j] * values[t + j]
                    out[t, pl.ds(row + 8 * q, 8, stride=TS // 8 * 4), :] = acc
            return 0

        lax.fori_loop(0, run.size, body, 0)

    def finish(group, rel):
        readers = sum(SIZES[UNITS[u][0]] for u in GROUPS[group])
        for side, flag in ((0, has_down), (1, has_up)):
            @pl.when(flag)
            def _():
                wait_in(halo.at[side, rel, pl.ds(0, readers)], h_recv.at[side, rel, group])
        for u in GROUPS[group]:
            sum_rows(u, rel)

    for kind, u in ORDER:
        if kind == "P":
            wait_in(plane.at[slots(u)], in_recv.at[u])
        elif kind == "S1":
            cross_copy(u).start()
        elif kind == "N":
            @pl.when(has_near)
            def _():
                near_halo(u).start()
        elif kind == "A":
            finish(u, 0)
        elif kind == "X":
            wait_in(cross.at[slots(u)], x_recv.at[u])
        elif kind == "B":
            finish(u, 1)
        else:
            @pl.when(has_far)
            def _():
                if kind == "Nf":
                    far_halo(u).start()
                elif kind == "F":
                    side_halo(u).start()
                elif kind == "W":
                    forward(u).start()
                elif kind == "R1":
                    wait_in(relay.at[1, slots(u)], r_recv.at[1, u])
                    relay_near(u, 0).start()
                elif kind == "R2":
                    wait_in(relay.at[2, slots(u)], r_recv.at[2, u])
                    relay_near(u, 1).start()
                elif kind == "R3":
                    wait_in(relay.at[0, slots(u)], r_recv.at[0, u])
                    relay_far(u).start()

    wait_out(plane.at[pl.ds(0, SLOTS - 1)], in_send)
    wait_out(cross, z_send.at[7])

    @pl.when(has_near)
    def _():
        wait_out(relay.at[0], z_send.at[0])

    @pl.when(has_far)
    def _():
        for kind in range(1, 7):
            wait_out(relay.at[0], z_send.at[kind])


def on_device(groups, frames, taps):
    shaped = frames.reshape(4, 8, 8, frames.shape[3])
    summed = pl.pallas_call(
        functools.partial(kernel, groups),
        out_shape=jax.ShapeDtypeStruct((4, 4 * TS, 128), jnp.float32),
        in_specs=[pl.BlockSpec(memory_space=pltpu.HBM), pl.BlockSpec(memory_space=pltpu.HBM)],
        out_specs=pl.BlockSpec(memory_space=pltpu.VMEM),
        scratch_shapes=[
            pltpu.SMEM((7,), jnp.float32),
            pltpu.VMEM((SLOTS, 4, 2, 8, TS), jnp.float32),
            pltpu.VMEM((SLOTS, 4, 8, TS), jnp.float32),
            pltpu.VMEM((3, SLOTS, 3, 8, TS), jnp.float32),
            pltpu.VMEM((2, 2, SLOTS, 3, 8, TS), jnp.float32),
            pltpu.SemaphoreType.DMA,
            pltpu.SemaphoreType.DMA,
            pltpu.SemaphoreType.REGULAR,
            pltpu.SemaphoreType.DMA,
            pltpu.SemaphoreType.DMA((STEPS,)),
            pltpu.SemaphoreType.DMA((STEPS,)),
            pltpu.SemaphoreType.DMA((8,)),
            pltpu.SemaphoreType.DMA((3, STEPS)),
            pltpu.SemaphoreType.DMA((2, 2, len(GROUPS))),
        ],
        compiler_params=pltpu.CompilerParams(
            collective_id=0, has_side_effects=True, vmem_limit_bytes=24 * 2**20
        ),
        name="exchange",
    )(
        pltpu.with_memory_space_constraint(taps, pltpu.HBM),
        pltpu.with_memory_space_constraint(shaped, pltpu.HBM),
    )
    tiled = summed.reshape(4, TS // 8, TS // 128, 8, 128)
    return tiled.transpose(0, 1, 3, 2, 4).reshape(1, 4, TS, TS)


def solution(mesh):
    placed = (P("ta", "sa", None, None), P())
    return jax.shard_map(
        functools.partial(on_device, mesh.shape["ta"]),
        mesh=mesh, in_specs=placed, out_specs=P("sa", "ta", None, None), check_vma=False,
    )
```

```python
import functools

import jax
import jax.numpy as jnp
from jax import lax
from jax.experimental import pallas as pl
from jax.experimental.pallas import tpu as pltpu
from jax.sharding import PartitionSpec as P

TS = 512
NX = 4
CHIPS = NX * NX
SLOTS = 2 * CHIPS
MESH = pl.DeviceIdType.MESH

UNITS = (
    ('one', 0, 0),
    ('one', 0, 1),
    ('one', 1, 0),
    ('one', 4, 0),
    ('one', 3, 0),
    ('one', 12, 0),
    ('one', 1, 1),
    ('one', 4, 1),
    ('one', 12, 1),
    ('one', 3, 1),
    ('chip', 2),
    ('chip', 5),
    ('chip', 13),
    ('pair', 8),
    ('pair', 6),
    ('pair', 14),
    ('pair', 10),
)
SENDS = (
    (0, 1),
    (1, 0),
    (4, 0),
    (3, 0),
    (12, 0),
    (1, 1),
    (4, 1),
    (3, 1),
    (12, 1),
    (5, 0),
    (5, 1),
    (13, 0),
    (13, 1),
    (2, 0),
    (2, 1),
    (8, 0),
    (8, 1),
    (9, 0),
    (9, 1),
    (6, 0),
    (6, 1),
    (7, 0),
    (7, 1),
    (14, 0),
    (14, 1),
    (15, 0),
    (15, 1),
    (10, 0),
    (10, 1),
    (11, 0),
    (11, 1),
)
CLOSE = tuple(t for t in SENDS if t[0] // 4 == 0 or t[0] % 4 == 0)
SIZES = {"one": 1, "chip": 2, "pair": 4}
STEPS = len(UNITS)
GROUPS = (tuple(range(2, 10)), (0, 1, 10, 11), (12, 13), (14,), (15,), (16,))
ROUND = (13,)
ROUND_SIZE = sum(SIZES[UNITS[u][0]] for u in ROUND)
GROUP_OF = {u: i for i, units in enumerate(GROUPS) for u in units}
LAGS = dict(P=0, S1=0, Nf=0, N=0, F=0, R1=1, R3=7, X=3, W=3, R2=42, A=56, B=56)
CHAIN = (("C1", 15), ("C2", 23), ("C3", 47), ("C4", 19), ("Q", 48), ("QS", 53))
ORDER = tuple(
    (kind, step - lag)
    for step in range(STEPS + max(LAGS.values()))
    for kind, lag in (LAGS | dict(CHAIN)).items()
    if 0 <= step - lag < (1 if kind in dict(CHAIN) else len(GROUPS) if kind in "AB" else STEPS)
    and (step > lag or kind not in ("P", "S1", "N", "Nf", "F"))
)


def unit_of(offset, other):
    for u, unit in enumerate(UNITS):
        if unit[0] == "one":
            hit = unit[1:] == (offset, other)
        elif unit[0] == "chip":
            hit = unit[1] == offset
        else:
            hit = unit[1] // 2 == offset // 2
        if hit:
            return u


def flipped(v, bits):
    return (v, v + 1 - 2 * (v % 2), (v + 2) % NX, NX - 1 - v)[bits]


def kernel(
    groups, taps_hbm, frames, out, taps_ref, plane, cross, relay, halo, chain, part,
    taps_sem, own_sem, row_sem, in_send, in_recv, x_recv, z_send, r_recv, h_recv, c_send, c_recv,
):
    g = lax.axis_index("ta")
    s = lax.axis_index("sa")
    c = s % 2
    x = (s // 2) % NX
    a = (s // (2 * NX)) % 2
    y = s // (4 * NX)
    mine = (y * NX + x) * 2 + c
    last = groups - 1
    step = 2 * a - 1
    beyond, near = (g + step + groups) % groups, g - step
    has_near = jnp.logical_and(near >= 0, near <= last)
    has_far = jnp.logical_and(g + step >= 0, g + step <= last)
    outer = jnp.logical_not(has_far)
    inner = jnp.logical_not(has_near)
    inner = jnp.logical_and(inner, has_far)
    middle = jnp.logical_and(has_near, has_far)
    adds = jnp.logical_and(middle, jnp.logical_or(beyond == 0, beyond == last))
    takes = jnp.logical_and(middle, jnp.logical_not(adds))
    has_up = g < last
    has_down = g > 0

    def device(group, yy, zz, xx, cc):
        return (group, ((yy * 2 + zz) * NX + xx) * 2 + cc)

    def chip(offset):
        return flipped(y, offset // NX), flipped(x, offset % NX)

    partner = device(g, y, 1 - a, x, c)
    beyond_chip = device(beyond, y, 1 - a, x, c)

    def slots(u):
        unit = UNITS[u]
        yy, xx = chip(unit[1])
        base = 2 * (yy * NX + xx)
        if unit[0] == "one":
            return pl.ds(base + (c if unit[2] == 0 else 1 - c), 1)
        if unit[0] == "pair":
            base = base // 4 * 4
        return pl.ds(base, SIZES[unit[0]])

    def piece(yy, xx, cc):
        return frames.at[:, pl.ds(2 * yy, 2), :, pl.ds(pl.multiple_of(TS * (2 * xx + cc), TS), TS)]

    own = pltpu.make_async_copy(piece(y, x, c), plane.at[mine], own_sem)
    own.start()
    weights = pltpu.make_async_copy(taps_hbm, taps_ref, taps_sem)
    weights.start()

    barrier = pltpu.get_barrier_semaphore()

    def signal(semaphore, target):
        pl.semaphore_signal(semaphore, inc=1, device_id=target, device_id_type=MESH)

    for offset, other in reversed(CLOSE):
        yy, xx = chip(offset)
        signal(barrier, device(g, yy, a, xx, (c + other) % 2))
    signal(barrier, partner)
    signal(barrier, beyond_chip)
    pl.semaphore_wait(barrier, len(CLOSE) + 2)

    def remote(src, dst, send, recv, target):
        return pltpu.make_async_remote_copy(
            src_ref=src, dst_ref=dst, send_sem=send, recv_sem=recv,
            device_id=target, device_id_type=MESH,
        )

    def in_plane(offset, other):
        yy, xx = chip(offset)
        cc = (c + other) % 2
        return remote(
            piece(yy, xx, cc), plane.at[mine], in_send, in_recv.at[unit_of(offset, other)],
            device(g, yy, a, xx, cc),
        )

    def cross_copy(u):
        return remote(
            plane.at[slots(u), :, 1 - a], cross.at[slots(u)], z_send.at[7], x_recv.at[u], partner
        )

    def near_halo(u):
        return remote(
            plane.at[slots(u), pl.ds(1 - a, 3), a], relay.at[0, slots(u)],
            z_send.at[0], r_recv.at[0, u], partner,
        )

    def far_halo(u):
        return remote(
            plane.at[slots(u), pl.ds(a, 3), a], relay.at[1, slots(u)],
            z_send.at[1], r_recv.at[1, u], beyond_chip,
        )

    def side_halo(u):
        return remote(
            plane.at[slots(u), pl.ds(a, 3), 1 - a], halo.at[1 - a, 1, slots(u)],
            z_send.at[2], h_recv.at[1 - a, 1, GROUP_OF[u]], beyond_chip,
        )

    def forward(u):
        return remote(
            cross.at[slots(u), pl.ds(a, 3)], relay.at[2, slots(u)],
            z_send.at[3], r_recv.at[2, u], beyond_chip,
        )

    def relay_near(u, w):
        return remote(
            relay.at[1 + w, slots(u)], halo.at[a, w, slots(u)],
            z_send.at[4 + w], h_recv.at[a, w, GROUP_OF[u]], partner,
        )

    def relay_far(u):
        return remote(
            relay.at[0, slots(u)], halo.at[1 - a, 0, slots(u)],
            z_send.at[6], h_recv.at[1 - a, 0, GROUP_OF[u]], beyond_chip,
        )

    def in_round(u):
        before = ROUND[: ROUND.index(u)]
        return pl.ds(sum(SIZES[UNITS[v][0]] for v in before), SIZES[UNITS[u][0]])

    def round_copy(hop, u=None):
        run = None if u is None else in_round(u)
        if hop == 0:
            return remote(
                plane.at[slots(u), pl.ds(1 - a, 3), 1 - a], chain.at[0, run],
                c_send, c_recv.at[0], beyond_chip,
            )
        if hop == 1:
            return remote(chain.at[0], chain.at[0], c_send, c_recv.at[0], partner)
        if hop == 2:
            return remote(chain.at[0], chain.at[1], c_send, c_recv.at[1], beyond_chip)
        if hop == 3:
            return remote(chain.at[1], chain.at[1], c_send, c_recv.at[1], partner)
        return remote(
            chain.at[1, run], halo.at[a, 1, slots(u)],
            c_send, h_recv.at[a, 1, GROUP_OF[u]], beyond_chip,
        )

    def part_copy(u):
        return remote(
            part.at[in_round(u)], cross.at[slots(u)], z_send.at[7], x_recv.at[u],
            partner,
        )

    def wait_in(ref, sem):
        remote(ref, ref, in_send, sem, partner).wait_recv()

    def wait_out(ref, sem):
        remote(ref, ref, sem, own_sem, partner).wait_send()


    for offset, other in CLOSE:
        in_plane(offset, other).start()
    for bits in range(1, NX):
        signal(row_sem, device(g, y, a, flipped(x, bits), c))

    own.wait()
    cross_copy(0).start()

    @pl.when(has_near)
    def _():
        near_halo(0).start()

    @pl.when(has_far)
    def _():
        far_halo(0).start()
        side_halo(0).start()

    pl.semaphore_wait(row_sem, NX - 1)
    for offset, other in SENDS:
        if (offset, other) not in CLOSE:
            in_plane(offset, other).start()

    def zero(side):
        def body(i, _):
            halo[side, i // SLOTS, i % SLOTS] = jnp.zeros((3, 8, TS), jnp.float32)
            return 0
        lax.fori_loop(0, 2 * SLOTS, body, 0)

    @pl.when(jnp.logical_not(has_down))
    def _():
        zero(0)

    @pl.when(jnp.logical_not(has_up))
    def _():
        zero(1)

    weights.wait()
    taps = [taps_ref[j] for j in range(7)]

    def sum_rows(u, rel):
        run = slots(u)

        def body(i, _):
            slot = run.start + i
            m = slot // 2
            z = a if rel == 0 else 1 - a
            row = ((m // NX) * 2 + z) * 32 + (m % NX) * 2 + slot % 2
            for q in range(TS // 128):
                lanes = pl.ds(q * 128, 128)
                values = [halo[0, rel, slot, j, :, lanes] for j in range(3)]
                if rel == 0:
                    values += [plane[slot, j, a, :, lanes] for j in range(4)]
                else:
                    values += [cross[slot, j, :, lanes] for j in range(4)]
                values += [halo[1, rel, slot, j, :, lanes] for j in range(3)]
                for t in range(4):
                    acc = taps[0] * values[t]
                    for j in range(1, 7):
                        acc = acc + taps[j] * values[t + j]
                    out[t, pl.ds(row + 8 * q, 8, stride=TS // 8 * 4), :] = acc
            return 0

        lax.fori_loop(0, run.size, body, 0)

    def add_up(u):
        def body(n, _):
            slot, i = slots(u).start + n // 4, in_round(u).start + n // 4
            lanes = pl.ds(pl.multiple_of(n % 4 * 128, 128), 128)
            steps = [plane[slot, j, 1 - a, :, lanes] for j in range(4)]
            past = [relay[2, slot, j, :, lanes] for j in range(3)]

            @pl.when(a == 0)
            def _():
                values = past + steps
                for t in range(4):
                    acc = taps[0] * values[t]
                    for j in range(1, 7 - t):
                        acc = acc + taps[j] * values[t + j]
                    part[i, t, :, lanes] = acc

            @pl.when(a == 1)
            def _():
                values = steps + past
                for t in range(4):
                    first = max(3 - t, 0)
                    acc = taps[first] * values[t + first - 3]
                    for j in range(first + 1, 7):
                        acc = acc + taps[j] * values[t + j - 3]
                    part[i, t, :, lanes] = acc

            return 0

        lax.fori_loop(0, 4 * slots(u).size, body, 0)

    def sum_part(u):
        def body(n, _):
            slot, q = slots(u).start + n // 4, n % 4
            m = slot // 2
            row = ((m // NX) * 2 + 1 - a) * 32 + (m % NX) * 2 + slot % 2
            lanes = pl.ds(pl.multiple_of(q * 128, 128), 128)
            begun = [cross[slot, t, :, lanes] for t in range(4)]
            rest = [halo[a, 1, slot, j, :, lanes] for j in range(3)]

            @pl.when(a == 1)
            def _():
                for t in range(4):
                    acc = begun[t]
                    for j in range(7 - t, 7):
                        acc = acc + taps[j] * rest[t + j - 7]
                    out[t, pl.ds(row + 8 * q, 8, stride=TS // 8 * 4), :] = acc

            @pl.when(a == 0)
            def _():
                for t in range(4):
                    acc = begun[t]
                    for j in range(0, 3 - t):
                        acc = acc + taps[j] * rest[t + j]
                    out[t, pl.ds(row + 8 * q, 8, stride=TS // 8 * 4), :] = acc

            return 0

        lax.fori_loop(0, 4 * slots(u).size, body, 0)

    def finish(group, rel):
        readers = sum(SIZES[UNITS[u][0]] for u in GROUPS[group])
        around = [u for u in GROUPS[group] if u in ROUND] if rel == 1 else []

        def wait_side(side, count):
            wait_in(halo.at[side, rel, pl.ds(0, count)], h_recv.at[side, rel, group])

        for side, flag in ((0, has_down), (1, has_up)):
            if around:
                fewer = jnp.logical_and(takes, a == 1 - side)

                @pl.when(fewer)
                def _():
                    wait_side(side, readers - ROUND_SIZE)

                flag = jnp.logical_and(flag, jnp.logical_not(fewer))

            @pl.when(flag)
            def _():
                wait_side(side, readers)

        for u in GROUPS[group]:
            if u in around:
                @pl.when(takes)
                def _():
                    wait_in(cross.at[slots(u)], x_recv.at[u])
                    sum_part(u)

                @pl.when(jnp.logical_not(takes))
                def _():
                    sum_rows(u, rel)
            else:
                sum_rows(u, rel)

    for kind, u in ORDER:
        if kind == "P":
            wait_in(plane.at[slots(u)], in_recv.at[u])
        elif kind == "S1":
            if u in ROUND:
                @pl.when(jnp.logical_not(adds))
                def _():
                    cross_copy(u).start()

                @pl.when(adds)
                def _():
                    round_copy(0, u).start()
            else:
                cross_copy(u).start()
        elif kind == "N":
            @pl.when(has_near)
            def _():
                near_halo(u).start()
        elif kind == "A":
            finish(u, 0)
        elif kind == "X":
            if u in ROUND:
                @pl.when(jnp.logical_not(takes))
                def _():
                    wait_in(cross.at[slots(u)], x_recv.at[u])
            else:
                wait_in(cross.at[slots(u)], x_recv.at[u])
        elif kind in ("C1", "C4"):
            @pl.when(inner)
            def _():
                way = 0 if kind == "C1" else 1
                wait_in(chain.at[way], c_recv.at[way])
                if kind == "C1":
                    round_copy(1).start()
                else:
                    for v in ROUND:
                        round_copy(4, v).start()
        elif kind in ("C2", "C3"):
            @pl.when(outer)
            def _():
                way = 0 if kind == "C2" else 1
                wait_in(chain.at[way], c_recv.at[way])
                round_copy(2 + way).start()
        elif kind == "Q":
            @pl.when(adds)
            def _():
                for v in ROUND:
                    wait_in(relay.at[2, slots(v)], r_recv.at[2, v])
                    add_up(v)
        elif kind == "QS":
            @pl.when(adds)
            def _():
                for v in ROUND:
                    part_copy(v).start()
        elif kind == "B":
            finish(u, 1)
        else:
            flag = has_far
            if u in ROUND and kind == "W":
                flag = jnp.logical_and(flag, jnp.logical_not(takes))
            if u in ROUND and kind == "R2":
                flag = jnp.logical_and(flag, jnp.logical_not(middle))

            @pl.when(flag)
            def _():
                if kind == "Nf":
                    far_halo(u).start()
                elif kind == "F":
                    side_halo(u).start()
                elif kind == "W":
                    forward(u).start()
                elif kind == "R1":
                    wait_in(relay.at[1, slots(u)], r_recv.at[1, u])
                    relay_near(u, 0).start()
                elif kind == "R2":
                    wait_in(relay.at[2, slots(u)], r_recv.at[2, u])
                    relay_near(u, 1).start()
                elif kind == "R3":
                    wait_in(relay.at[0, slots(u)], r_recv.at[0, u])
                    relay_far(u).start()

    wait_out(plane.at[pl.ds(0, SLOTS - 1)], in_send)
    wait_out(cross, z_send.at[7])

    @pl.when(has_near)
    def _():
        wait_out(relay.at[0], z_send.at[0])

    few = SLOTS - ROUND_SIZE

    @pl.when(has_far)
    def _():
        for kind in (1, 2, 4, 6):
            wait_out(relay.at[0], z_send.at[kind])

        for kind, fewer in ((3, takes), (5, middle)):
            @pl.when(fewer)
            def _():
                wait_out(relay.at[0, pl.ds(0, few)], z_send.at[kind])

            @pl.when(jnp.logical_not(fewer))
            def _():
                wait_out(relay.at[0], z_send.at[kind])

    @pl.when(adds)
    def _():
        wait_out(chain.at[0], c_send)

    @pl.when(jnp.logical_or(inner, outer))
    def _():
        wait_out(chain, c_send)


def on_device(groups, frames, taps):
    shaped = frames.reshape(4, 8, 8, frames.shape[3])
    summed = pl.pallas_call(
        functools.partial(kernel, groups),
        out_shape=jax.ShapeDtypeStruct((4, 4 * TS, 128), jnp.float32),
        in_specs=[pl.BlockSpec(memory_space=pltpu.HBM), pl.BlockSpec(memory_space=pltpu.HBM)],
        out_specs=pl.BlockSpec(memory_space=pltpu.VMEM),
        scratch_shapes=[
            pltpu.SMEM((7,), jnp.float32),
            pltpu.VMEM((SLOTS, 4, 2, 8, TS), jnp.float32),
            pltpu.VMEM((SLOTS, 4, 8, TS), jnp.float32),
            pltpu.VMEM((3, SLOTS, 3, 8, TS), jnp.float32),
            pltpu.VMEM((2, 2, SLOTS, 3, 8, TS), jnp.float32),
            pltpu.VMEM((2, ROUND_SIZE, 3, 8, TS), jnp.float32),
            pltpu.VMEM((ROUND_SIZE, 4, 8, TS), jnp.float32),
            pltpu.SemaphoreType.DMA,
            pltpu.SemaphoreType.DMA,
            pltpu.SemaphoreType.REGULAR,
            pltpu.SemaphoreType.DMA,
            pltpu.SemaphoreType.DMA((STEPS,)),
            pltpu.SemaphoreType.DMA((STEPS,)),
            pltpu.SemaphoreType.DMA((8,)),
            pltpu.SemaphoreType.DMA((3, STEPS)),
            pltpu.SemaphoreType.DMA((2, 2, len(GROUPS))),
            pltpu.SemaphoreType.DMA,
            pltpu.SemaphoreType.DMA((2,)),
        ],
        compiler_params=pltpu.CompilerParams(
            collective_id=0, has_side_effects=True, vmem_limit_bytes=24 * 2**20
        ),
        name="exchange",
    )(
        pltpu.with_memory_space_constraint(taps, pltpu.HBM),
        pltpu.with_memory_space_constraint(shaped, pltpu.HBM),
    )
    tiled = summed.reshape(4, TS // 8, TS // 128, 8, 128)
    return tiled.transpose(0, 1, 3, 2, 4).reshape(1, 4, TS, TS)


def solution(mesh):
    placed = (P("ta", "sa", None, None), P())
    return jax.shard_map(
        functools.partial(on_device, mesh.shape["ta"]),
        mesh=mesh, in_specs=placed, out_specs=P("sa", "ta", None, None), check_vma=False,
    )
```

```python
import functools

import jax
import jax.numpy as jnp
from jax import lax
from jax.experimental import pallas as pl
from jax.experimental.pallas import tpu as pltpu
from jax.sharding import PartitionSpec as P

TS = 512
NX = 4
CHIPS = NX * NX
SLOTS = 2 * CHIPS
MESH = pl.DeviceIdType.MESH

UNITS = (
    ('one', 0, 0),
    ('one', 0, 1),
    ('one', 1, 0),
    ('one', 4, 0),
    ('one', 3, 0),
    ('one', 12, 0),
    ('one', 1, 1),
    ('one', 4, 1),
    ('one', 12, 1),
    ('one', 3, 1),
    ('chip', 2),
    ('chip', 5),
    ('chip', 13),
    ('pair', 8),
    ('pair', 6),
    ('pair', 14),
    ('pair', 10),
)
SENDS = (
    (0, 1),
    (1, 0),
    (4, 0),
    (3, 0),
    (12, 0),
    (1, 1),
    (4, 1),
    (3, 1),
    (12, 1),
    (5, 0),
    (5, 1),
    (13, 0),
    (13, 1),
    (2, 0),
    (2, 1),
    (8, 0),
    (8, 1),
    (9, 0),
    (9, 1),
    (6, 0),
    (6, 1),
    (7, 0),
    (7, 1),
    (14, 0),
    (14, 1),
    (15, 0),
    (15, 1),
    (10, 0),
    (10, 1),
    (11, 0),
    (11, 1),
)
CLOSE = tuple(t for t in SENDS if t[0] // 4 == 0 or t[0] % 4 == 0)
SIZES = {"one": 1, "chip": 2, "pair": 4}
STEPS = len(UNITS)
GROUPS = (tuple(range(2, 10)), (0, 1, 10, 11), (12, 13), (14,), (15,), (16,))
ROUND = (9, 13)
ROUND_SIZE = sum(SIZES[UNITS[u][0]] for u in ROUND)
GROUP_OF = {u: i for i, units in enumerate(GROUPS) for u in units}
LAGS = dict(P=0, S1=0, Nf=0, N=0, F=0, R1=1, R3=7, X=3, W=3, R2=42, A=56, B=56)
CHAIN = (("C1", 15), ("C2", 23), ("C3", 47), ("C4", 19), ("Q", 48), ("QS", 53))
ORDER = tuple(
    (kind, step - lag)
    for step in range(STEPS + max(LAGS.values()))
    for kind, lag in (LAGS | dict(CHAIN)).items()
    if 0 <= step - lag < (1 if kind in dict(CHAIN) else len(GROUPS) if kind in "AB" else STEPS)
    and (step > lag or kind not in ("P", "S1", "N", "Nf", "F"))
)


def unit_of(offset, other):
    for u, unit in enumerate(UNITS):
        if unit[0] == "one":
            hit = unit[1:] == (offset, other)
        elif unit[0] == "chip":
            hit = unit[1] == offset
        else:
            hit = unit[1] // 2 == offset // 2
        if hit:
            return u


def flipped(v, bits):
    return (v, v + 1 - 2 * (v % 2), (v + 2) % NX, NX - 1 - v)[bits]


def kernel(
    groups, taps_hbm, frames, out, taps_ref, plane, cross, relay, halo, chain, part,
    taps_sem, own_sem, row_sem, in_send, in_recv, x_recv, z_send, r_recv, h_recv, c_send, c_recv,
):
    g = lax.axis_index("ta")
    s = lax.axis_index("sa")
    c = s % 2
    x = (s // 2) % NX
    a = (s // (2 * NX)) % 2
    y = s // (4 * NX)
    mine = (y * NX + x) * 2 + c
    last = groups - 1
    step = 2 * a - 1
    beyond, near = (g + step + groups) % groups, g - step
    has_near = jnp.logical_and(near >= 0, near <= last)
    has_far = jnp.logical_and(g + step >= 0, g + step <= last)
    outer = jnp.logical_not(has_far)
    inner = jnp.logical_not(has_near)
    inner = jnp.logical_and(inner, has_far)
    middle = jnp.logical_and(has_near, has_far)
    adds = jnp.logical_and(middle, jnp.logical_or(beyond == 0, beyond == last))
    takes = jnp.logical_and(middle, jnp.logical_not(adds))
    has_up = g < last
    has_down = g > 0

    def device(group, yy, zz, xx, cc):
        return (group, ((yy * 2 + zz) * NX + xx) * 2 + cc)

    def chip(offset):
        return flipped(y, offset // NX), flipped(x, offset % NX)

    partner = device(g, y, 1 - a, x, c)
    beyond_chip = device(beyond, y, 1 - a, x, c)

    def slots(u):
        unit = UNITS[u]
        yy, xx = chip(unit[1])
        base = 2 * (yy * NX + xx)
        if unit[0] == "one":
            return pl.ds(base + (c if unit[2] == 0 else 1 - c), 1)
        if unit[0] == "pair":
            base = base // 4 * 4
        return pl.ds(base, SIZES[unit[0]])

    def piece(yy, xx, cc):
        return frames.at[:, pl.ds(2 * yy, 2), :, pl.ds(pl.multiple_of(TS * (2 * xx + cc), TS), TS)]

    own = pltpu.make_async_copy(piece(y, x, c), plane.at[mine], own_sem)
    own.start()
    weights = pltpu.make_async_copy(taps_hbm, taps_ref, taps_sem)
    weights.start()

    barrier = pltpu.get_barrier_semaphore()

    def signal(semaphore, target):
        pl.semaphore_signal(semaphore, inc=1, device_id=target, device_id_type=MESH)

    for offset, other in reversed(CLOSE):
        yy, xx = chip(offset)
        signal(barrier, device(g, yy, a, xx, (c + other) % 2))
    signal(barrier, partner)
    signal(barrier, beyond_chip)
    pl.semaphore_wait(barrier, len(CLOSE) + 2)

    def remote(src, dst, send, recv, target):
        return pltpu.make_async_remote_copy(
            src_ref=src, dst_ref=dst, send_sem=send, recv_sem=recv,
            device_id=target, device_id_type=MESH,
        )

    def in_plane(offset, other):
        yy, xx = chip(offset)
        cc = (c + other) % 2
        return remote(
            piece(yy, xx, cc), plane.at[mine], in_send, in_recv.at[unit_of(offset, other)],
            device(g, yy, a, xx, cc),
        )

    def cross_copy(u):
        return remote(
            plane.at[slots(u), :, 1 - a], cross.at[slots(u)], z_send.at[7], x_recv.at[u], partner
        )

    def near_halo(u):
        return remote(
            plane.at[slots(u), pl.ds(1 - a, 3), a], relay.at[0, slots(u)],
            z_send.at[0], r_recv.at[0, u], partner,
        )

    def far_halo(u):
        return remote(
            plane.at[slots(u), pl.ds(a, 3), a], relay.at[1, slots(u)],
            z_send.at[1], r_recv.at[1, u], beyond_chip,
        )

    def side_halo(u):
        return remote(
            plane.at[slots(u), pl.ds(a, 3), 1 - a], halo.at[1 - a, 1, slots(u)],
            z_send.at[2], h_recv.at[1 - a, 1, GROUP_OF[u]], beyond_chip,
        )

    def forward(u):
        return remote(
            cross.at[slots(u), pl.ds(a, 3)], relay.at[2, slots(u)],
            z_send.at[3], r_recv.at[2, u], beyond_chip,
        )

    def relay_near(u, w):
        return remote(
            relay.at[1 + w, slots(u)], halo.at[a, w, slots(u)],
            z_send.at[4 + w], h_recv.at[a, w, GROUP_OF[u]], partner,
        )

    def relay_far(u):
        return remote(
            relay.at[0, slots(u)], halo.at[1 - a, 0, slots(u)],
            z_send.at[6], h_recv.at[1 - a, 0, GROUP_OF[u]], beyond_chip,
        )

    def in_round(u):
        before = ROUND[: ROUND.index(u)]
        return pl.ds(sum(SIZES[UNITS[v][0]] for v in before), SIZES[UNITS[u][0]])

    def round_copy(hop, u=None):
        run = None if u is None else in_round(u)
        if hop == 0:
            return remote(
                plane.at[slots(u), pl.ds(1 - a, 3), 1 - a], chain.at[0, run],
                c_send, c_recv.at[0], beyond_chip,
            )
        if hop == 1:
            return remote(chain.at[0], chain.at[0], c_send, c_recv.at[0], partner)
        if hop == 2:
            return remote(chain.at[0], chain.at[1], c_send, c_recv.at[1], beyond_chip)
        if hop == 3:
            return remote(chain.at[1], chain.at[1], c_send, c_recv.at[1], partner)
        return remote(
            chain.at[1, run], halo.at[a, 1, slots(u)],
            c_send, h_recv.at[a, 1, GROUP_OF[u]], beyond_chip,
        )

    def part_copy(u):
        return remote(
            part.at[in_round(u)], cross.at[slots(u)], z_send.at[7], x_recv.at[u],
            partner,
        )

    def wait_in(ref, sem):
        remote(ref, ref, in_send, sem, partner).wait_recv()

    def wait_out(ref, sem):
        remote(ref, ref, sem, own_sem, partner).wait_send()


    for offset, other in CLOSE:
        in_plane(offset, other).start()
    for bits in range(1, NX):
        signal(row_sem, device(g, y, a, flipped(x, bits), c))

    own.wait()
    cross_copy(0).start()

    @pl.when(has_near)
    def _():
        near_halo(0).start()

    @pl.when(has_far)
    def _():
        far_halo(0).start()
        side_halo(0).start()

    pl.semaphore_wait(row_sem, NX - 1)
    for offset, other in SENDS:
        if (offset, other) not in CLOSE:
            in_plane(offset, other).start()

    def zero(side):
        def body(i, _):
            halo[side, i // SLOTS, i % SLOTS] = jnp.zeros((3, 8, TS), jnp.float32)
            return 0
        lax.fori_loop(0, 2 * SLOTS, body, 0)

    @pl.when(jnp.logical_not(has_down))
    def _():
        zero(0)

    @pl.when(jnp.logical_not(has_up))
    def _():
        zero(1)

    weights.wait()
    taps = [taps_ref[j] for j in range(7)]

    def sum_rows(u, rel):
        run = slots(u)

        def body(i, _):
            slot = run.start + i
            m = slot // 2
            z = a if rel == 0 else 1 - a
            row = ((m // NX) * 2 + z) * 32 + (m % NX) * 2 + slot % 2
            for q in range(TS // 128):
                lanes = pl.ds(q * 128, 128)
                values = [halo[0, rel, slot, j, :, lanes] for j in range(3)]
                if rel == 0:
                    values += [plane[slot, j, a, :, lanes] for j in range(4)]
                else:
                    values += [cross[slot, j, :, lanes] for j in range(4)]
                values += [halo[1, rel, slot, j, :, lanes] for j in range(3)]
                for t in range(4):
                    acc = taps[0] * values[t]
                    for j in range(1, 7):
                        acc = acc + taps[j] * values[t + j]
                    out[t, pl.ds(row + 8 * q, 8, stride=TS // 8 * 4), :] = acc
            return 0

        lax.fori_loop(0, run.size, body, 0)

    def add_up(u):
        def body(n, _):
            slot, i = slots(u).start + n // 4, in_round(u).start + n // 4
            lanes = pl.ds(pl.multiple_of(n % 4 * 128, 128), 128)
            steps = [plane[slot, j, 1 - a, :, lanes] for j in range(4)]
            past = [relay[2, slot, j, :, lanes] for j in range(3)]

            @pl.when(a == 0)
            def _():
                values = past + steps
                for t in range(4):
                    acc = taps[0] * values[t]
                    for j in range(1, 7 - t):
                        acc = acc + taps[j] * values[t + j]
                    part[i, t, :, lanes] = acc

            @pl.when(a == 1)
            def _():
                values = steps + past
                for t in range(4):
                    first = max(3 - t, 0)
                    acc = taps[first] * values[t + first - 3]
                    for j in range(first + 1, 7):
                        acc = acc + taps[j] * values[t + j - 3]
                    part[i, t, :, lanes] = acc

            return 0

        lax.fori_loop(0, 4 * slots(u).size, body, 0)

    def sum_part(u):
        def body(n, _):
            slot, q = slots(u).start + n // 4, n % 4
            m = slot // 2
            row = ((m // NX) * 2 + 1 - a) * 32 + (m % NX) * 2 + slot % 2
            lanes = pl.ds(pl.multiple_of(q * 128, 128), 128)
            begun = [cross[slot, t, :, lanes] for t in range(4)]
            rest = [halo[a, 1, slot, j, :, lanes] for j in range(3)]

            @pl.when(a == 1)
            def _():
                for t in range(4):
                    acc = begun[t]
                    for j in range(7 - t, 7):
                        acc = acc + taps[j] * rest[t + j - 7]
                    out[t, pl.ds(row + 8 * q, 8, stride=TS // 8 * 4), :] = acc

            @pl.when(a == 0)
            def _():
                for t in range(4):
                    acc = begun[t]
                    for j in range(0, 3 - t):
                        acc = acc + taps[j] * rest[t + j]
                    out[t, pl.ds(row + 8 * q, 8, stride=TS // 8 * 4), :] = acc

            return 0

        lax.fori_loop(0, 4 * slots(u).size, body, 0)

    def finish(group, rel):
        readers = sum(SIZES[UNITS[u][0]] for u in GROUPS[group])
        around = [u for u in GROUPS[group] if u in ROUND] if rel == 1 else []

        def wait_side(side, count):
            wait_in(halo.at[side, rel, pl.ds(0, count)], h_recv.at[side, rel, group])

        for side, flag in ((0, has_down), (1, has_up)):
            if around:
                fewer = jnp.logical_and(takes, a == 1 - side)

                @pl.when(fewer)
                def _():
                    wait_side(side, readers - sum(SIZES[UNITS[u][0]] for u in around))

                flag = jnp.logical_and(flag, jnp.logical_not(fewer))

            @pl.when(flag)
            def _():
                wait_side(side, readers)

        for u in GROUPS[group]:
            if u in around:
                @pl.when(takes)
                def _():
                    wait_in(cross.at[slots(u)], x_recv.at[u])
                    sum_part(u)

                @pl.when(jnp.logical_not(takes))
                def _():
                    sum_rows(u, rel)
            else:
                sum_rows(u, rel)

    for kind, u in ORDER:
        if kind == "P":
            wait_in(plane.at[slots(u)], in_recv.at[u])
        elif kind == "S1":
            if u in ROUND:
                @pl.when(jnp.logical_not(adds))
                def _():
                    cross_copy(u).start()

                @pl.when(adds)
                def _():
                    round_copy(0, u).start()
            else:
                cross_copy(u).start()
        elif kind == "N":
            @pl.when(has_near)
            def _():
                near_halo(u).start()
        elif kind == "A":
            finish(u, 0)
        elif kind == "X":
            if u in ROUND:
                @pl.when(jnp.logical_not(takes))
                def _():
                    wait_in(cross.at[slots(u)], x_recv.at[u])
            else:
                wait_in(cross.at[slots(u)], x_recv.at[u])
        elif kind in ("C1", "C4"):
            @pl.when(inner)
            def _():
                way = 0 if kind == "C1" else 1
                wait_in(chain.at[way], c_recv.at[way])
                if kind == "C1":
                    round_copy(1).start()
                else:
                    for v in ROUND:
                        round_copy(4, v).start()
        elif kind in ("C2", "C3"):
            @pl.when(outer)
            def _():
                way = 0 if kind == "C2" else 1
                wait_in(chain.at[way], c_recv.at[way])
                round_copy(2 + way).start()
        elif kind == "Q":
            @pl.when(adds)
            def _():
                for v in ROUND:
                    wait_in(relay.at[2, slots(v)], r_recv.at[2, v])
                    add_up(v)
        elif kind == "QS":
            @pl.when(adds)
            def _():
                for v in ROUND:
                    part_copy(v).start()
        elif kind == "B":
            finish(u, 1)
        else:
            flag = has_far
            if u in ROUND and kind == "W":
                flag = jnp.logical_and(flag, jnp.logical_not(takes))
            if u in ROUND and kind == "R2":
                flag = jnp.logical_and(flag, jnp.logical_not(middle))

            @pl.when(flag)
            def _():
                if kind == "Nf":
                    far_halo(u).start()
                elif kind == "F":
                    side_halo(u).start()
                elif kind == "W":
                    forward(u).start()
                elif kind == "R1":
                    wait_in(relay.at[1, slots(u)], r_recv.at[1, u])
                    relay_near(u, 0).start()
                elif kind == "R2":
                    wait_in(relay.at[2, slots(u)], r_recv.at[2, u])
                    relay_near(u, 1).start()
                elif kind == "R3":
                    wait_in(relay.at[0, slots(u)], r_recv.at[0, u])
                    relay_far(u).start()

    wait_out(plane.at[pl.ds(0, SLOTS - 1)], in_send)
    wait_out(cross, z_send.at[7])

    @pl.when(has_near)
    def _():
        wait_out(relay.at[0], z_send.at[0])

    few = SLOTS - ROUND_SIZE

    @pl.when(has_far)
    def _():
        for kind in (1, 2, 4, 6):
            wait_out(relay.at[0], z_send.at[kind])

        for kind, fewer in ((3, takes), (5, middle)):
            @pl.when(fewer)
            def _():
                wait_out(relay.at[0, pl.ds(0, few)], z_send.at[kind])

            @pl.when(jnp.logical_not(fewer))
            def _():
                wait_out(relay.at[0], z_send.at[kind])

    @pl.when(adds)
    def _():
        wait_out(chain.at[0], c_send)

    @pl.when(jnp.logical_or(inner, outer))
    def _():
        wait_out(chain, c_send)


def on_device(groups, frames, taps):
    shaped = frames.reshape(4, 8, 8, frames.shape[3])
    summed = pl.pallas_call(
        functools.partial(kernel, groups),
        out_shape=jax.ShapeDtypeStruct((4, 4 * TS, 128), jnp.float32),
        in_specs=[pl.BlockSpec(memory_space=pltpu.HBM), pl.BlockSpec(memory_space=pltpu.HBM)],
        out_specs=pl.BlockSpec(memory_space=pltpu.VMEM),
        scratch_shapes=[
            pltpu.SMEM((7,), jnp.float32),
            pltpu.VMEM((SLOTS, 4, 2, 8, TS), jnp.float32),
            pltpu.VMEM((SLOTS, 4, 8, TS), jnp.float32),
            pltpu.VMEM((3, SLOTS, 3, 8, TS), jnp.float32),
            pltpu.VMEM((2, 2, SLOTS, 3, 8, TS), jnp.float32),
            pltpu.VMEM((2, ROUND_SIZE, 3, 8, TS), jnp.float32),
            pltpu.VMEM((ROUND_SIZE, 4, 8, TS), jnp.float32),
            pltpu.SemaphoreType.DMA,
            pltpu.SemaphoreType.DMA,
            pltpu.SemaphoreType.REGULAR,
            pltpu.SemaphoreType.DMA,
            pltpu.SemaphoreType.DMA((STEPS,)),
            pltpu.SemaphoreType.DMA((STEPS,)),
            pltpu.SemaphoreType.DMA((8,)),
            pltpu.SemaphoreType.DMA((3, STEPS)),
            pltpu.SemaphoreType.DMA((2, 2, len(GROUPS))),
            pltpu.SemaphoreType.DMA,
            pltpu.SemaphoreType.DMA((2,)),
        ],
        compiler_params=pltpu.CompilerParams(
            collective_id=0, has_side_effects=True, vmem_limit_bytes=24 * 2**20
        ),
        name="exchange",
    )(
        pltpu.with_memory_space_constraint(taps, pltpu.HBM),
        pltpu.with_memory_space_constraint(shaped, pltpu.HBM),
    )
    tiled = summed.reshape(4, TS // 8, TS // 128, 8, 128)
    return tiled.transpose(0, 1, 3, 2, 4).reshape(1, 4, TS, TS)


def solution(mesh):
    placed = (P("ta", "sa", None, None), P())
    return jax.shard_map(
        functools.partial(on_device, mesh.shape["ta"]),
        mesh=mesh, in_specs=placed, out_specs=P("sa", "ta", None, None), check_vma=False,
    )
```

```python
import functools

import jax
import jax.numpy as jnp
from jax import lax
from jax.experimental import pallas as pl
from jax.experimental.pallas import tpu as pltpu
from jax.sharding import PartitionSpec as P

TS = 512
NX = 4
CHIPS = NX * NX
SLOTS = 2 * CHIPS
MESH = pl.DeviceIdType.MESH

UNITS = (
    ('one', 0, 0),
    ('one', 0, 1),
    ('one', 1, 0),
    ('one', 4, 0),
    ('one', 3, 0),
    ('one', 12, 0),
    ('one', 1, 1),
    ('one', 4, 1),
    ('one', 12, 1),
    ('one', 3, 1),
    ('chip', 2),
    ('chip', 5),
    ('chip', 13),
    ('pair', 8),
    ('pair', 6),
    ('pair', 14),
    ('pair', 10),
)
SENDS = (
    (0, 1),
    (1, 0),
    (4, 0),
    (3, 0),
    (12, 0),
    (1, 1),
    (4, 1),
    (3, 1),
    (12, 1),
    (5, 0),
    (5, 1),
    (13, 0),
    (13, 1),
    (2, 0),
    (2, 1),
    (8, 0),
    (8, 1),
    (9, 0),
    (9, 1),
    (6, 0),
    (6, 1),
    (7, 0),
    (7, 1),
    (14, 0),
    (14, 1),
    (15, 0),
    (15, 1),
    (10, 0),
    (10, 1),
    (11, 0),
    (11, 1),
)
CLOSE = tuple(t for t in SENDS if t[0] // 4 == 0 or t[0] % 4 == 0)
SIZES = {"one": 1, "chip": 2, "pair": 4}
STEPS = len(UNITS)
GROUPS = (tuple(range(2, 10)), (0, 1, 10, 11), (12, 13), (14,), (15,), (16,))
ROUND = (9, 13)
ROUND_SIZE = sum(SIZES[UNITS[u][0]] for u in ROUND)
GROUP_OF = {u: i for i, units in enumerate(GROUPS) for u in units}
LAGS = dict(P=0, S1=0, Nf=0, N=0, F=0, R1=1, R3=7, X=3, W=3, R2=42, A=59, B=59)
CHAIN = (("C1", 15), ("C2", 23), ("C3", 47), ("C4", 19), ("Q", 48), ("QS", 53))
ORDER = tuple(
    (kind, step - lag)
    for step in range(STEPS + max(LAGS.values()))
    for kind, lag in (LAGS | dict(CHAIN)).items()
    if 0 <= step - lag < (1 if kind in dict(CHAIN) else len(GROUPS) if kind in "AB" else STEPS)
    and (step > lag or kind not in ("P", "S1", "N", "Nf", "F"))
)


def unit_of(offset, other):
    for u, unit in enumerate(UNITS):
        if unit[0] == "one":
            hit = unit[1:] == (offset, other)
        elif unit[0] == "chip":
            hit = unit[1] == offset
        else:
            hit = unit[1] // 2 == offset // 2
        if hit:
            return u


def flipped(v, bits):
    return (v, v + 1 - 2 * (v % 2), (v + 2) % NX, NX - 1 - v)[bits]


def kernel(
    groups, taps_hbm, frames, out, taps_ref, plane, cross, relay, halo, chain, part,
    taps_sem, own_sem, row_sem, in_send, in_recv, x_recv, z_send, r_recv, h_recv, c_send, c_recv,
):
    g = lax.axis_index("ta")
    s = lax.axis_index("sa")
    c = s % 2
    x = (s // 2) % NX
    a = (s // (2 * NX)) % 2
    y = s // (4 * NX)
    mine = (y * NX + x) * 2 + c
    last = groups - 1
    step = 2 * a - 1
    beyond, near = (g + step + groups) % groups, g - step
    has_near = jnp.logical_and(near >= 0, near <= last)
    has_far = jnp.logical_and(g + step >= 0, g + step <= last)
    outer = jnp.logical_not(has_far)
    inner = jnp.logical_not(has_near)
    inner = jnp.logical_and(inner, has_far)
    middle = jnp.logical_and(has_near, has_far)
    adds = jnp.logical_and(middle, jnp.logical_or(beyond == 0, beyond == last))
    takes = jnp.logical_and(middle, jnp.logical_not(adds))
    has_up = g < last
    has_down = g > 0

    def device(group, yy, zz, xx, cc):
        return (group, ((yy * 2 + zz) * NX + xx) * 2 + cc)

    def chip(offset):
        return flipped(y, offset // NX), flipped(x, offset % NX)

    partner = device(g, y, 1 - a, x, c)
    beyond_chip = device(beyond, y, 1 - a, x, c)

    def slots(u):
        unit = UNITS[u]
        yy, xx = chip(unit[1])
        base = 2 * (yy * NX + xx)
        if unit[0] == "one":
            return pl.ds(base + (c if unit[2] == 0 else 1 - c), 1)
        if unit[0] == "pair":
            base = base // 4 * 4
        return pl.ds(base, SIZES[unit[0]])

    def piece(yy, xx, cc):
        return frames.at[:, pl.ds(2 * yy, 2), :, pl.ds(pl.multiple_of(TS * (2 * xx + cc), TS), TS)]

    own = pltpu.make_async_copy(piece(y, x, c), plane.at[mine], own_sem)
    own.start()
    weights = pltpu.make_async_copy(taps_hbm, taps_ref, taps_sem)
    weights.start()

    barrier = pltpu.get_barrier_semaphore()

    def signal(semaphore, target):
        pl.semaphore_signal(semaphore, inc=1, device_id=target, device_id_type=MESH)

    for offset, other in reversed(CLOSE):
        yy, xx = chip(offset)
        signal(barrier, device(g, yy, a, xx, (c + other) % 2))
    signal(barrier, partner)
    signal(barrier, beyond_chip)
    pl.semaphore_wait(barrier, len(CLOSE) + 2)

    def remote(src, dst, send, recv, target):
        return pltpu.make_async_remote_copy(
            src_ref=src, dst_ref=dst, send_sem=send, recv_sem=recv,
            device_id=target, device_id_type=MESH,
        )

    def in_plane(offset, other):
        yy, xx = chip(offset)
        cc = (c + other) % 2
        return remote(
            piece(yy, xx, cc), plane.at[mine], in_send, in_recv.at[unit_of(offset, other)],
            device(g, yy, a, xx, cc),
        )

    def cross_copy(u):
        return remote(
            plane.at[slots(u), :, 1 - a], cross.at[slots(u)], z_send.at[7], x_recv.at[u], partner
        )

    def near_halo(u):
        return remote(
            plane.at[slots(u), pl.ds(1 - a, 3), a], relay.at[0, slots(u)],
            z_send.at[0], r_recv.at[0, u], partner,
        )

    def far_halo(u):
        return remote(
            plane.at[slots(u), pl.ds(a, 3), a], relay.at[1, slots(u)],
            z_send.at[1], r_recv.at[1, u], beyond_chip,
        )

    def side_halo(u):
        return remote(
            plane.at[slots(u), pl.ds(a, 3), 1 - a], halo.at[1 - a, 1, slots(u)],
            z_send.at[2], h_recv.at[1 - a, 1, GROUP_OF[u]], beyond_chip,
        )

    def forward(u):
        return remote(
            cross.at[slots(u), pl.ds(a, 3)], relay.at[2, slots(u)],
            z_send.at[3], r_recv.at[2, u], beyond_chip,
        )

    def relay_near(u, w):
        return remote(
            relay.at[1 + w, slots(u)], halo.at[a, w, slots(u)],
            z_send.at[4 + w], h_recv.at[a, w, GROUP_OF[u]], partner,
        )

    def relay_far(u):
        return remote(
            relay.at[0, slots(u)], halo.at[1 - a, 0, slots(u)],
            z_send.at[6], h_recv.at[1 - a, 0, GROUP_OF[u]], beyond_chip,
        )

    def in_round(u):
        before = ROUND[: ROUND.index(u)]
        return pl.ds(sum(SIZES[UNITS[v][0]] for v in before), SIZES[UNITS[u][0]])

    def round_copy(hop, u=None):
        run = None if u is None else in_round(u)
        if hop == 0:
            return remote(
                plane.at[slots(u), pl.ds(1 - a, 3), 1 - a], chain.at[0, run],
                c_send, c_recv.at[0], beyond_chip,
            )
        if hop == 1:
            return remote(chain.at[0], chain.at[0], c_send, c_recv.at[0], partner)
        if hop == 2:
            return remote(chain.at[0], chain.at[1], c_send, c_recv.at[1], beyond_chip)
        if hop == 3:
            return remote(chain.at[1], chain.at[1], c_send, c_recv.at[1], partner)
        return remote(
            chain.at[1, run], halo.at[a, 1, slots(u)],
            c_send, h_recv.at[a, 1, GROUP_OF[u]], beyond_chip,
        )

    def part_copy(u):
        return remote(
            part.at[in_round(u)], cross.at[slots(u)], z_send.at[7], x_recv.at[u],
            partner,
        )

    def wait_in(ref, sem):
        remote(ref, ref, in_send, sem, partner).wait_recv()

    def wait_out(ref, sem):
        remote(ref, ref, sem, own_sem, partner).wait_send()


    for offset, other in CLOSE:
        in_plane(offset, other).start()
    for bits in range(1, NX):
        signal(row_sem, device(g, y, a, flipped(x, bits), c))

    own.wait()
    cross_copy(0).start()

    @pl.when(has_near)
    def _():
        near_halo(0).start()

    @pl.when(has_far)
    def _():
        far_halo(0).start()
        side_halo(0).start()

    pl.semaphore_wait(row_sem, NX - 1)
    for offset, other in SENDS:
        if (offset, other) not in CLOSE:
            in_plane(offset, other).start()

    def zero(side):
        def body(i, _):
            halo[side, i // SLOTS, i % SLOTS] = jnp.zeros((3, 8, TS), jnp.float32)
            return 0
        lax.fori_loop(0, 2 * SLOTS, body, 0)

    @pl.when(jnp.logical_not(has_down))
    def _():
        zero(0)

    @pl.when(jnp.logical_not(has_up))
    def _():
        zero(1)

    weights.wait()
    taps = [taps_ref[j] for j in range(7)]

    def sum_rows(u, rel):
        run = slots(u)

        def body(i, _):
            slot = run.start + i
            m = slot // 2
            z = a if rel == 0 else 1 - a
            row = ((m // NX) * 2 + z) * 32 + (m % NX) * 2 + slot % 2
            for q in range(TS // 128):
                lanes = pl.ds(q * 128, 128)
                values = [halo[0, rel, slot, j, :, lanes] for j in range(3)]
                if rel == 0:
                    values += [plane[slot, j, a, :, lanes] for j in range(4)]
                else:
                    values += [cross[slot, j, :, lanes] for j in range(4)]
                values += [halo[1, rel, slot, j, :, lanes] for j in range(3)]
                for t in range(4):
                    acc = taps[0] * values[t]
                    for j in range(1, 7):
                        acc = acc + taps[j] * values[t + j]
                    out[t, pl.ds(row + 8 * q, 8, stride=TS // 8 * 4), :] = acc
            return 0

        lax.fori_loop(0, run.size, body, 0)

    def add_up(u):
        def body(n, _):
            slot, i = slots(u).start + n // 4, in_round(u).start + n // 4
            lanes = pl.ds(pl.multiple_of(n % 4 * 128, 128), 128)
            steps = [plane[slot, j, 1 - a, :, lanes] for j in range(4)]
            past = [relay[2, slot, j, :, lanes] for j in range(3)]

            @pl.when(a == 0)
            def _():
                values = past + steps
                for t in range(4):
                    acc = taps[0] * values[t]
                    for j in range(1, 7 - t):
                        acc = acc + taps[j] * values[t + j]
                    part[i, t, :, lanes] = acc

            @pl.when(a == 1)
            def _():
                values = steps + past
                for t in range(4):
                    first = max(3 - t, 0)
                    acc = taps[first] * values[t + first - 3]
                    for j in range(first + 1, 7):
                        acc = acc + taps[j] * values[t + j - 3]
                    part[i, t, :, lanes] = acc

            return 0

        lax.fori_loop(0, 4 * slots(u).size, body, 0)

    def sum_part(u):
        def body(n, _):
            slot, q = slots(u).start + n // 4, n % 4
            m = slot // 2
            row = ((m // NX) * 2 + 1 - a) * 32 + (m % NX) * 2 + slot % 2
            lanes = pl.ds(pl.multiple_of(q * 128, 128), 128)
            begun = [cross[slot, t, :, lanes] for t in range(4)]
            rest = [halo[a, 1, slot, j, :, lanes] for j in range(3)]

            @pl.when(a == 1)
            def _():
                for t in range(4):
                    acc = begun[t]
                    for j in range(7 - t, 7):
                        acc = acc + taps[j] * rest[t + j - 7]
                    out[t, pl.ds(row + 8 * q, 8, stride=TS // 8 * 4), :] = acc

            @pl.when(a == 0)
            def _():
                for t in range(4):
                    acc = begun[t]
                    for j in range(0, 3 - t):
                        acc = acc + taps[j] * rest[t + j]
                    out[t, pl.ds(row + 8 * q, 8, stride=TS // 8 * 4), :] = acc

            return 0

        lax.fori_loop(0, 4 * slots(u).size, body, 0)

    def finish(group, rel):
        readers = sum(SIZES[UNITS[u][0]] for u in GROUPS[group])
        around = [u for u in GROUPS[group] if u in ROUND] if rel == 1 else []

        def wait_side(side, count):
            wait_in(halo.at[side, rel, pl.ds(0, count)], h_recv.at[side, rel, group])

        for side, flag in ((0, has_down), (1, has_up)):
            if around:
                fewer = jnp.logical_and(takes, a == 1 - side)

                @pl.when(fewer)
                def _():
                    wait_side(side, readers - sum(SIZES[UNITS[u][0]] for u in around))

                flag = jnp.logical_and(flag, jnp.logical_not(fewer))

            @pl.when(flag)
            def _():
                wait_side(side, readers)

        for u in GROUPS[group]:
            if u in around:
                @pl.when(takes)
                def _():
                    wait_in(cross.at[slots(u)], x_recv.at[u])
                    sum_part(u)

                @pl.when(jnp.logical_not(takes))
                def _():
                    sum_rows(u, rel)
            else:
                sum_rows(u, rel)

    for kind, u in ORDER:
        if kind == "P":
            wait_in(plane.at[slots(u)], in_recv.at[u])
        elif kind == "S1":
            if u in ROUND:
                @pl.when(jnp.logical_not(adds))
                def _():
                    cross_copy(u).start()

                @pl.when(adds)
                def _():
                    round_copy(0, u).start()
            else:
                cross_copy(u).start()
        elif kind == "N":
            @pl.when(has_near)
            def _():
                near_halo(u).start()
        elif kind == "A":
            finish(u, 0)
        elif kind == "X":
            if u in ROUND:
                @pl.when(jnp.logical_not(takes))
                def _():
                    wait_in(cross.at[slots(u)], x_recv.at[u])
            else:
                wait_in(cross.at[slots(u)], x_recv.at[u])
        elif kind in ("C1", "C4"):
            @pl.when(inner)
            def _():
                way = 0 if kind == "C1" else 1
                wait_in(chain.at[way], c_recv.at[way])
                if kind == "C1":
                    round_copy(1).start()
                else:
                    for v in ROUND:
                        round_copy(4, v).start()
        elif kind in ("C2", "C3"):
            @pl.when(outer)
            def _():
                way = 0 if kind == "C2" else 1
                wait_in(chain.at[way], c_recv.at[way])
                round_copy(2 + way).start()
        elif kind == "Q":
            @pl.when(adds)
            def _():
                for v in ROUND:
                    wait_in(relay.at[2, slots(v)], r_recv.at[2, v])
                    add_up(v)
        elif kind == "QS":
            @pl.when(adds)
            def _():
                for v in ROUND:
                    part_copy(v).start()
        elif kind == "B":
            finish(u, 1)
        else:
            flag = has_far
            if u in ROUND and kind == "W":
                flag = jnp.logical_and(flag, jnp.logical_not(takes))
            if u in ROUND and kind == "R2":
                flag = jnp.logical_and(flag, jnp.logical_not(middle))

            @pl.when(flag)
            def _():
                if kind == "Nf":
                    far_halo(u).start()
                elif kind == "F":
                    side_halo(u).start()
                elif kind == "W":
                    forward(u).start()
                elif kind == "R1":
                    wait_in(relay.at[1, slots(u)], r_recv.at[1, u])
                    relay_near(u, 0).start()
                elif kind == "R2":
                    wait_in(relay.at[2, slots(u)], r_recv.at[2, u])
                    relay_near(u, 1).start()
                elif kind == "R3":
                    wait_in(relay.at[0, slots(u)], r_recv.at[0, u])
                    relay_far(u).start()

    wait_out(plane.at[pl.ds(0, SLOTS - 1)], in_send)
    wait_out(cross, z_send.at[7])

    @pl.when(has_near)
    def _():
        wait_out(relay.at[0], z_send.at[0])

    few = SLOTS - ROUND_SIZE

    @pl.when(has_far)
    def _():
        for kind in (1, 2, 4, 6):
            wait_out(relay.at[0], z_send.at[kind])

        for kind, fewer in ((3, takes), (5, middle)):
            @pl.when(fewer)
            def _():
                wait_out(relay.at[0, pl.ds(0, few)], z_send.at[kind])

            @pl.when(jnp.logical_not(fewer))
            def _():
                wait_out(relay.at[0], z_send.at[kind])

    @pl.when(adds)
    def _():
        wait_out(chain.at[0], c_send)

    @pl.when(jnp.logical_or(inner, outer))
    def _():
        wait_out(chain, c_send)


def on_device(groups, frames, taps):
    shaped = frames.reshape(4, 8, 8, frames.shape[3])
    summed = pl.pallas_call(
        functools.partial(kernel, groups),
        out_shape=jax.ShapeDtypeStruct((4, 4 * TS, 128), jnp.float32),
        in_specs=[pl.BlockSpec(memory_space=pltpu.HBM), pl.BlockSpec(memory_space=pltpu.HBM)],
        out_specs=pl.BlockSpec(memory_space=pltpu.VMEM),
        scratch_shapes=[
            pltpu.SMEM((7,), jnp.float32),
            pltpu.VMEM((SLOTS, 4, 2, 8, TS), jnp.float32),
            pltpu.VMEM((SLOTS, 4, 8, TS), jnp.float32),
            pltpu.VMEM((3, SLOTS, 3, 8, TS), jnp.float32),
            pltpu.VMEM((2, 2, SLOTS, 3, 8, TS), jnp.float32),
            pltpu.VMEM((2, ROUND_SIZE, 3, 8, TS), jnp.float32),
            pltpu.VMEM((ROUND_SIZE, 4, 8, TS), jnp.float32),
            pltpu.SemaphoreType.DMA,
            pltpu.SemaphoreType.DMA,
            pltpu.SemaphoreType.REGULAR,
            pltpu.SemaphoreType.DMA,
            pltpu.SemaphoreType.DMA((STEPS,)),
            pltpu.SemaphoreType.DMA((STEPS,)),
            pltpu.SemaphoreType.DMA((8,)),
            pltpu.SemaphoreType.DMA((3, STEPS)),
            pltpu.SemaphoreType.DMA((2, 2, len(GROUPS))),
            pltpu.SemaphoreType.DMA,
            pltpu.SemaphoreType.DMA((2,)),
        ],
        compiler_params=pltpu.CompilerParams(
            collective_id=0, has_side_effects=True, vmem_limit_bytes=24 * 2**20
        ),
        name="exchange",
    )(
        pltpu.with_memory_space_constraint(taps, pltpu.HBM),
        pltpu.with_memory_space_constraint(shaped, pltpu.HBM),
    )
    tiled = summed.reshape(4, TS // 8, TS // 128, 8, 128)
    return tiled.transpose(0, 1, 3, 2, 4).reshape(1, 4, TS, TS)


def solution(mesh):
    placed = (P("ta", "sa", None, None), P())
    return jax.shard_map(
        functools.partial(on_device, mesh.shape["ta"]),
        mesh=mesh, in_specs=placed, out_specs=P("sa", "ta", None, None), check_vma=False,
    )
```
